256 devices in a mesh: groups: 2 (over y), ctx: 128 (over x, z, core).
Axes of the slice: x: 4, y: 2, z: 16, core: 2. Of those that a mesh axis runs over, the one named last changes fastest.
The devices are a block of a 4x16x16 slice.
Arguments:
- queries: bfloat16 [256, 8192], P(('groups', 'ctx')), parts along dimension 0, may hold values from -120 to 120
- fresh_keys: bfloat16 [256, 512], P(('groups', 'ctx')), parts along dimension 0, may hold values from -4 to 4
- fresh_values: bfloat16 [256, 512], P(('groups', 'ctx')), parts along dimension 0, may hold values from -4 to 4
- cache_keys: bfloat16 [262144, 512], P(('groups', 'ctx')), parts along dimension 0, may hold values from -4 to 4
- stored_values: bfloat16 [262144, 512], P(('groups', 'ctx')), parts along dimension 0, may hold values from -4 to 4
- cache_lengths: int32 [256], P(('groups', 'ctx')), parts along dimension 0, may hold values from 1 to 1024, as said below
- positions: int32 [256], P('groups'), parts along dimension 0, may hold values from 0 to 127, each once
Outputs:
- attended: bfloat16 [256, 8192], P(('groups', 'ctx')), parts along dimension 0
The draws below stay inside these ranges and needn't reach their ends.
There are 2 independent parts, one for each index of `groups`. The reference program is written for one: setup_inputs(seed, part) draws one part's arguments, and reference() takes and returns one part's arrays. A program takes and returns all parts, laid end to end along the dimension named above; each array names one. Nothing has to cross between parts.
Inputs may be any that keep to these rules, and one draw needn't show every extreme that they name: `cache_lengths`: each entry lies between 1 and 1024, and one shard has all 1024 slots live.
All inputs are finite; a program needn't handle non-finite values.
Results may differ from the reference program's by a relative error of at most 0.003.
Values may be sent and summed in bfloat16 or wider, within the bound.
No kernel may reach another device: no remote copies, remote signals or barrier semaphores. Data moves between devices by JAX's collectives and lax.ppermute only.
A program may use at most 128 MiB of HBM per device.

```python
import jax
import jax.numpy as jnp
from jax import lax

KEY_VALUE_HEADS = 4
HEADS_PER_GROUP = 16
HEAD_WIDTH = 128
QUERY_HEADS = 64
NEW_DEV = 1
CACHE_DEV = 1024
NEW_TOKENS = 128
CACHE_SLOTS = 131072
N_CTX = 128


def full_shard(key):
    return jax.random.randint(jax.random.fold_in(key, 7), (), 0, N_CTX)


def key_table(key):
    return jnp.clip(jax.random.normal(jax.random.fold_in(key, 21), (CACHE_SLOTS, KEY_VALUE_HEADS * HEAD_WIDTH), jnp.float32), -4.0, 4.0)


def draw_cache_lengths(key, part):
    first = jax.random.randint(jax.random.fold_in(key, 11), (N_CTX,), 1, CACHE_DEV + 1)
    second = jax.random.randint(jax.random.fold_in(key, 12), (N_CTX,), 1, CACHE_DEV + 1)
    lengths = jnp.maximum(first * second // CACHE_DEV, 1)
    lengths = jnp.where(jnp.arange(N_CTX) == full_shard(key), CACHE_DEV, lengths)
    return lengths.astype(jnp.int32)


def draw_cache_keys(key, part):
    lookup_table = key_table(key)
    return lookup_table.astype(jnp.bfloat16)


def draw_queries(key, part):
    base = 2.5 * jnp.clip(jax.random.normal(jax.random.fold_in(key, 31), (NEW_TOKENS, QUERY_HEADS * HEAD_WIDTH), jnp.float32), -4.0, 4.0)
    return base.astype(jnp.bfloat16)


def block_levels(stream_key, extent, split, low, high):
    loudness, own = 1.0, jax.random.fold_in(stream_key, 6)
    for position, shards_of in split:
        draws = jnp.exp(jax.random.uniform(jax.random.fold_in(own, position), (shards_of,), jnp.float32, low / len(split), high / len(split)))
        loudness = loudness * jnp.repeat(draws, extent[position] // shards_of).reshape([-1 if axis == position else 1 for axis in range(len(extent))])
    return loudness


def centred(stream_key, dims, deviation, limit, pieces=(), kind=jnp.bfloat16):
    drawn = deviation * jax.random.normal(stream_key, dims, jnp.float32)
    if pieces:
        drawn = drawn * block_levels(stream_key, dims, pieces, -0.22, 0.18)
    return jnp.clip(drawn, -limit, limit).astype(kind)


def setup_inputs(seed: int = 0, part: int = 0) -> dict:
    key_list = jax.random.split(jax.random.key(seed), 8)
    part_keys = jax.random.split(jax.random.fold_in(key_list[7], part), 8)
    return {
        "queries": draw_queries(jax.random.fold_in(jax.random.fold_in(key_list[7], part), 71), part),
        "fresh_keys": centred(part_keys[1], (NEW_TOKENS, KEY_VALUE_HEADS * HEAD_WIDTH), 1.0, 4.0, ((0, 128),)),
        "fresh_values": centred(part_keys[2], (NEW_TOKENS, KEY_VALUE_HEADS * HEAD_WIDTH), 1.0, 4.0, ((0, 128),)),
        "cache_keys": draw_cache_keys(jax.random.fold_in(jax.random.fold_in(key_list[7], part), 71), part),
        "stored_values": centred(part_keys[4], (CACHE_SLOTS, KEY_VALUE_HEADS * HEAD_WIDTH), 1.0, 4.0, ((0, 128),)),
        "cache_lengths": draw_cache_lengths(jax.random.fold_in(jax.random.fold_in(key_list[7], part), 71), part),
        "positions": jax.random.permutation(part_keys[6], NEW_TOKENS).astype(jnp.int32),
    }


def block_partials(queries, keys_of_block, values_of_block, visible):
    slice_width = keys_of_block.shape[0]
    query_float = queries.astype(jnp.float32).reshape(NEW_TOKENS, KEY_VALUE_HEADS, HEADS_PER_GROUP, HEAD_WIDTH)
    key_float = keys_of_block.astype(jnp.float32).reshape(slice_width, KEY_VALUE_HEADS, HEAD_WIDTH)
    value_float = values_of_block.astype(jnp.float32).reshape(slice_width, KEY_VALUE_HEADS, HEAD_WIDTH)
    scores = jnp.einsum("nhgd,khd->nhgk", query_float, key_float) * (HEAD_WIDTH ** -0.5)
    scores = jnp.where(visible[:, None, None, :], scores, -jnp.inf)
    maxima = jnp.max(scores, axis=-1)
    weights = jnp.exp(scores - maxima[..., None]).astype(jnp.bfloat16)
    totals = jnp.sum(weights.astype(jnp.float32), axis=-1)
    sums = jnp.einsum("nhgk,khd->nhgd", weights.astype(jnp.float32), value_float)
    return maxima.reshape(NEW_TOKENS, QUERY_HEADS), totals.reshape(NEW_TOKENS, QUERY_HEADS), sums.reshape(NEW_TOKENS, QUERY_HEADS, HEAD_WIDTH)


def reference(queries, fresh_keys, fresh_values, cache_keys, stored_values, cache_lengths, positions):
    def step(carry, block):
        run_max, run_sum, run_total = carry
        first = (block * CACHE_DEV).astype(jnp.int32)
        second = (block * NEW_DEV).astype(jnp.int32)
        keys_of_block = jnp.concatenate([lax.dynamic_slice_in_dim(cache_keys, first, CACHE_DEV, 0), lax.dynamic_slice_in_dim(fresh_keys, second, NEW_DEV, 0)], axis=0)
        values_of_block = jnp.concatenate([lax.dynamic_slice_in_dim(stored_values, first, CACHE_DEV, 0), lax.dynamic_slice_in_dim(fresh_values, second, NEW_DEV, 0)], axis=0)
        key_order = lax.dynamic_slice_in_dim(positions, second, NEW_DEV, 0)
        live = jnp.arange(CACHE_DEV, dtype=jnp.int32) < cache_lengths[block]
        cache_seen = jnp.broadcast_to(live[None, :], (NEW_TOKENS, CACHE_DEV))
        new_seen = key_order[None, :] <= positions[:, None]
        visible = jnp.concatenate([cache_seen, new_seen], axis=1)
        maxima, totals, sums = block_partials(queries, keys_of_block, values_of_block, visible)
        top = jnp.maximum(run_max, maxima)
        old_scale = jnp.exp(run_max - top)
        new_scale = jnp.exp(maxima - top)
        run_sum = run_sum * old_scale[..., None] + sums * new_scale[..., None]
        run_total = run_total * old_scale + totals * new_scale
        return (top, run_sum, run_total), None

    start = (jnp.full((NEW_TOKENS, QUERY_HEADS), -jnp.inf, jnp.float32), jnp.zeros((NEW_TOKENS, QUERY_HEADS, HEAD_WIDTH), jnp.float32), jnp.zeros((NEW_TOKENS, QUERY_HEADS), jnp.float32))
    (run_max, run_sum, run_total), unused = lax.scan(step, start, jnp.arange(N_CTX, dtype=jnp.int32))
    result = run_sum / run_total[..., None]
    return result.reshape(NEW_TOKENS, QUERY_HEADS * HEAD_WIDTH).astype(jnp.bfloat16)
```

```python
import functools
import math

import jax
import jax.numpy as jnp
from jax import lax
from jax.experimental import pallas as pl
from jax.experimental.pallas import tpu as pltpu
from jax.sharding import Mesh
from jax.sharding import PartitionSpec as P

HEADS_PER_GROUP = 16
HEAD_WIDTH = 128
GROUPS_CTX = ("groups", "x", "z", "core")
NX, NZ = 4, 16
LOG2_SCALE = HEAD_WIDTH ** (-0.5) * math.log2(math.e)
STAT_ROWS = 8
LSE_STEPS = 2.0**18
FULL = 32767.0
F32, BF16, I16, I32 = jnp.float32, jnp.bfloat16, jnp.int16, jnp.int32
SWAP = [(0, 1), (1, 0)]


def dot_nt(a, b):
    return lax.dot_general(a, b, (((1,), (1,)), ((), ())), preferred_element_type=F32)


def dot_nn(a, b):
    return lax.dot_general(a, b, (((1,), (0,)), ((), ())), preferred_element_type=F32)


def diagonal(rows):
    row = lax.broadcasted_iota(jnp.int32, (rows, 128), 0)
    lane = lax.broadcasted_iota(jnp.int32, (rows, 128), 1)
    return lax.rem(lane, rows) == row


def attend_kernel(len_ref, q_ref, k_ref, v_ref, kn_ref, vn_ref, bias_ref, o_ref, s_scr, sn_scr, acc_scr, m_scr, st_scr):
    tokens, kv_heads, group = q_ref.shape[:3]
    rows = tokens * group
    slots = k_ref.shape[2]
    tile = chunk = 256
    chunks = o_ref.shape[0]
    per = rows // chunks

    @pl.loop(0, kv_heads)
    def head(kv):
        @pl.loop(0, 2)
        def block(blk):
            live = len_ref[blk]

            def variant(n):
                for r in range(0, rows, tile):
                    t0, t1 = r // group, (r + tile) // group
                    q = q_ref[t0:t1, kv].reshape(tile, HEAD_WIDTH)
                    bias = bias_ref[blk, t0:t1]
                    bias = jnp.broadcast_to(bias[:, None, :], (t1 - t0, group, 128)).reshape(tile, 128)
                    s_new = dot_nt(q, kn_ref[kv]) + bias
                    sn_scr[r : r + tile] = s_new
                    top = s_new
                    for c in range(0, n, chunk):
                        s = dot_nt(q, k_ref[blk, kv, c : c + chunk, :])
                        if c + chunk > (n // 2 if n > chunk else 0):
                            col = lax.broadcasted_iota(jnp.int32, (1, chunk), 1) + c
                            s = s + jnp.where(col < live, 0.0, -jnp.inf)
                        s_scr[r : r + tile, c : c + chunk] = s
                        for l in range(0, chunk, 128):
                            top = jnp.maximum(top, s[:, l : l + 128])
                    top = jnp.max(top, axis=1, keepdims=True)
                    acc = None
                    for c in range(0, n, chunk):
                        p = jnp.exp2((s_scr[r : r + tile, c : c + chunk] - top) * LOG2_SCALE).astype(BF16)
                        v = v_ref[blk, kv, c : c + chunk, :]
                        term = dot_nn(p, jnp.concatenate([v, jnp.ones_like(v)], axis=1))
                        acc = term if acc is None else acc + term
                    p = jnp.exp2((sn_scr[r : r + tile] - top) * LOG2_SCALE).astype(BF16)
                    v = vn_ref[kv]
                    acc = acc + dot_nn(p, jnp.concatenate([v, jnp.ones_like(v)], axis=1))
                    acc_scr[blk, r : r + tile, :] = acc
                    m_scr[blk, r : r + tile, :] = jnp.broadcast_to(top * LOG2_SCALE, (tile, 128))

            low = 0
            for n in (slots // 4, slots // 2, slots):
                pl.when(jnp.logical_and(live > low, live <= n))(functools.partial(variant, n))
                low = n

        m_a, m_b = m_scr[0], m_scr[1]
        top = jnp.maximum(m_a, m_b)
        w_a, w_b = jnp.exp2(m_a - top), jnp.exp2(m_b - top)
        total = acc_scr[0, :, HEAD_WIDTH:] * w_a + acc_scr[1, :, HEAD_WIDTH:] * w_b
        mean = (acc_scr[0, :, :HEAD_WIDTH] * w_a + acc_scr[1, :, :HEAD_WIDTH] * w_b) / total
        lse = top + jnp.log2(total)
        at = pl.multiple_of(kv * per, per)
        coded, exponent = encode(mean)
        o_ref[:, pl.ds(at, per), :] = coded.reshape(chunks, per, HEAD_WIDTH).astype(I16)
        pick = diagonal(per)[None]
        st_scr[0, kv] = jnp.sum(jnp.where(pick, lse.reshape(chunks, per, 128), 0.0), axis=1)
        spread = jnp.broadcast_to(exponent, (rows, 128)).reshape(chunks, per, 128)
        st_scr[1, kv] = jnp.sum(jnp.where(pick, spread, 0.0), axis=1)

    write_stats(o_ref, [st_scr[0, kv] for kv in range(kv_heads)], [st_scr[1, kv] for kv in range(kv_heads)])


def encode(mean):
    largest = jnp.max(jnp.abs(mean), axis=-1, keepdims=True)
    exponent = jnp.ceil(jnp.log2(jnp.maximum(largest, 1e-30)))
    return jnp.round(mean * (FULL * jnp.exp2(-exponent))).astype(I32), exponent


def write_stats(o_ref, lses, exponents):
    steps = [jnp.round(l * LSE_STEPS).astype(I32) for l in lses]
    terms = [lax.shift_right_arithmetic(t, jnp.full_like(t, 16)) for t in steps]
    terms += [(t & 0xFFFF) - 32768 for t in steps]
    terms += [e.astype(I32) for e in exponents]
    terms += [jnp.zeros_like(terms[0])] * (STAT_ROWS - len(terms))
    rows = o_ref.shape[1] - STAT_ROWS
    o_ref[:, rows:, :] = jnp.stack(terms, axis=1).astype(I16)


def read_stats(stats):
    stats = stats.astype(I32)
    steps = stats[:, 0:2] * 65536 + (stats[:, 2:4] + 32768)
    return steps.astype(F32) * (1.0 / LSE_STEPS), jnp.exp2(stats[:, 4:6].astype(F32)) * (1.0 / FULL)


def as_column(w, per):
    chunks = w.shape[0]
    spread = jnp.broadcast_to(w[:, :, None, :], (chunks, 2, per, 128))
    lane = lax.broadcasted_iota(jnp.int32, (per, 128), 1)
    row = lax.broadcasted_iota(jnp.int32, (per, 128), 0)
    column = jnp.sum(jnp.where((lane == row)[None, None], spread, 0.0), axis=3, keepdims=True)
    return column.reshape(chunks, 2 * per, 1)


def numbers(coded):
    return coded.astype(I32).astype(F32)


def merge_kernel(*refs):
    pieces, o_ref = refs[:-1], refs[-1]
    rows = o_ref.shape[1] - STAT_ROWS
    lses, scales = zip(*[read_stats(p[:, rows:, :]) for p in pieces])
    top = functools.reduce(jnp.maximum, lses)
    weights = [jnp.exp2(l - top) for l in lses]
    total = functools.reduce(jnp.add, weights)
    lse = top + jnp.log2(total)
    out = None
    for p, w, scale in zip(pieces, weights, scales):
        term = numbers(p[:, :rows, :]) * as_column(w / total * scale, rows // 2)
        out = term if out is None else out + term
    coded, exponent = encode(out)
    o_ref[:, :rows, :] = coded.astype(I16)
    chunks, per = out.shape[0], rows // 2
    spread = jnp.broadcast_to(exponent, (chunks, rows, 128)).reshape(chunks, 2, per, 128)
    exponents = jnp.sum(jnp.where(diagonal(per)[None, None], spread, 0.0), axis=2)
    write_stats(o_ref, [lse[:, kv] for kv in range(2)], [exponents[:, kv] for kv in range(2)])


def final_kernel(p_ref, o_ref):
    rows = o_ref.shape[0]
    lse, scale = read_stats(p_ref[:, rows:, :])
    top = jnp.max(lse, axis=0, keepdims=True)
    weights = jnp.exp2(lse - top)
    weights = weights / jnp.sum(weights, axis=0, keepdims=True)
    column = as_column(weights * scale, rows // 2)
    o_ref[...] = jnp.sum(numbers(p_ref[:, :rows, :]) * column, axis=0).astype(BF16)


def attend(lengths, q, keys, values, new_keys, new_values, bias):
    tokens, kv_heads, group, width = q.shape
    rows = tokens * group
    slots = keys.shape[2]
    chunk_rows = rows // NZ * kv_heads
    vmem = pl.BlockSpec(memory_space=pltpu.VMEM)
    return pl.pallas_call(
        attend_kernel,
        out_shape=jax.ShapeDtypeStruct((NZ, chunk_rows + STAT_ROWS, width), I16),
        in_specs=[pl.BlockSpec(memory_space=pltpu.SMEM)] + [vmem] * 6,
        out_specs=vmem,
        scratch_shapes=[
            pltpu.VMEM((rows, slots), F32),
            pltpu.VMEM((rows, 128), F32),
            pltpu.VMEM((2, rows, 2 * width), F32),
            pltpu.VMEM((2, rows, 128), F32),
            pltpu.VMEM((2, kv_heads, NZ, 128), F32),
        ],
        compiler_params=pltpu.CompilerParams(vmem_limit_bytes=32 * 1024 * 1024),
        cost_estimate=pl.CostEstimate(
            flops=4 * rows * kv_heads * slots * 2 * width,
            bytes_accessed=2 * (keys.size + values.size),
            transcendentals=rows * kv_heads * slots,
        ),
        name="attend",
    )(lengths, q, keys, values, new_keys, new_values, bias)


def merge(pieces):
    return pl.pallas_call(
        merge_kernel,
        out_shape=jax.ShapeDtypeStruct(pieces[0].shape, I16),
        in_specs=[pl.BlockSpec(memory_space=pltpu.VMEM)] * len(pieces),
        out_specs=pl.BlockSpec(memory_space=pltpu.VMEM),
        cost_estimate=pl.CostEstimate(flops=8 * pieces[0].size, bytes_accessed=10 * pieces[0].size, transcendentals=0),
        name="merge",
    )(*pieces)


def finish(pieces):
    return pl.pallas_call(
        final_kernel,
        out_shape=jax.ShapeDtypeStruct((pieces.shape[1] - STAT_ROWS, HEAD_WIDTH), BF16),
        in_specs=[pl.BlockSpec(memory_space=pltpu.VMEM)],
        out_specs=pl.BlockSpec(memory_space=pltpu.VMEM),
        cost_estimate=pl.CostEstimate(flops=4 * pieces.size, bytes_accessed=2 * pieces.size, transcendentals=0),
        name="finish",
    )(pieces)


def along_x(a, step):
    return lax.ppermute(a, "x", [(i, (i - step) % NX) for i in range(NX)])


def body(queries, fresh_keys, fresh_values, cache_keys, stored_values, cache_lengths, positions):
    x, z, core = lax.axis_index("x"), lax.axis_index("z"), lax.axis_index("core")
    width, group = HEAD_WIDTH, HEADS_PER_GROUP
    kv_mine = fresh_keys.shape[1] // width // 2
    slots = cache_keys.shape[0]

    def halves(a):
        half = a.shape[1] // 2
        first, second = a[:, :half], a[:, half:]
        return jnp.where(core == 0, first, second), jnp.where(core == 0, second, first)

    keep, give = halves(queries)
    got = lax.ppermute(give, "core", SWAP)
    mine = jnp.stack([keep, got]).reshape(2, kv_mine, group, width)

    k_keep, k_give = halves(cache_keys)
    v_keep, v_give = halves(stored_values)

    def by_head(a):
        return a.reshape(a.shape[0], kv_mine, width).transpose(1, 0, 2)

    kv_keep = jnp.stack([by_head(k_keep), by_head(v_keep)])
    kv_give = jnp.stack([by_head(k_give), by_head(v_give)])
    kv_got = lax.ppermute(kv_give, "core", SWAP)
    keys = jnp.stack([kv_keep[0], kv_got[0]])
    values = jnp.stack([kv_keep[1], kv_got[1]])
    new_keep, new_give = halves(jnp.concatenate([fresh_keys, fresh_values], axis=0))
    new_got = lax.ppermute(new_give, "core", SWAP)
    new = jnp.stack([new_keep, new_got])
    new = new.reshape(2, 2, kv_mine, width).transpose(1, 2, 0, 3)
    new = jnp.pad(new, ((0, 0), (0, 0), (0, 128 - 2), (0, 0)))
    lengths = jnp.concatenate([cache_lengths, lax.ppermute(cache_lengths, "core", SWAP)])

    table = positions.reshape(NX, NZ, 2)
    table = jnp.where(core == 0, table, table[:, :, ::-1])
    here = lax.dynamic_slice(table, (x, z, 0), (1, 1, 2)).reshape(2)
    lane = jnp.arange(128, dtype=jnp.int32)

    def bias_of(step):
        there = lax.dynamic_slice(table, (lax.rem(x + step, NX), 0, 0), (1, NZ, 2)).reshape(1, NZ * 2, 1)
        seen = (here[:, None, None] <= there) & (lane[None, None, :] == jnp.arange(2)[:, None, None])
        return jnp.where(seen, 0.0, -jnp.inf).astype(F32)

    column = lax.all_to_all(jnp.broadcast_to(mine[None], (NZ, *mine.shape)), "z", 0, 0, tiled=True)
    column = column.reshape(NZ * 2, kv_mine, group, width)
    steps = (0, 1, 3, 2)
    asked = [column if s == 0 else along_x(column, s) for s in steps]
    results = [attend(lengths, q, keys, values, new[0], new[1], bias_of(s)) for q, s in zip(asked, steps)]
    pieces = [r if s == 0 else along_x(r, -s) for r, s in zip(results, steps)]
    merged = merge(pieces)
    merged = lax.all_to_all(merged, "z", 0, 0, tiled=True)
    done = finish(merged).reshape(kv_mine, 2, group * width)
    own, other = done[:, 0].reshape(1, -1), done[:, 1].reshape(1, -1)
    back = lax.ppermute(other, "core", SWAP)
    return jnp.where(core == 0, jnp.concatenate([own, back], 1), jnp.concatenate([back, own], 1))


def solution(mesh):
    finer = Mesh(mesh.devices.reshape(mesh.shape["groups"], NX, NZ, 2), GROUPS_CTX)
    return jax.shard_map(
        body,
        mesh=finer,
        in_specs=(
            P(GROUPS_CTX, None),
            P(GROUPS_CTX, None),
            P(GROUPS_CTX, None),
            P(GROUPS_CTX, None),
            P(GROUPS_CTX, None),
            P(GROUPS_CTX),
            P("groups"),
        ),
        out_specs=P(GROUPS_CTX, None),
        check_vma=False,
    )
```

```python
import functools
import math

import jax
import jax.numpy as jnp
from jax import lax
from jax.experimental import pallas as pl
from jax.experimental.pallas import tpu as pltpu
from jax.sharding import Mesh
from jax.sharding import PartitionSpec as P

HEADS_PER_GROUP = 16
HEAD_WIDTH = 128
GROUPS_CTX = ("groups", "x", "z", "core")
NX, NZ = 4, 16
LOG2_SCALE = HEAD_WIDTH ** (-0.5) * math.log2(math.e)
STAT_ROWS = 8
LSE_STEPS = 2.0**18
FULL = 32767.0
F32, BF16, I16, I32 = jnp.float32, jnp.bfloat16, jnp.int16, jnp.int32
SWAP = [(0, 1), (1, 0)]
CHUNK = 256
HIDDEN = -(2.0**100)


def dot_nt(a, b):
    return lax.dot_general(a, b, (((1,), (1,)), ((), ())), preferred_element_type=F32)


def dot_nn(a, b):
    return lax.dot_general(a, b, (((1,), (0,)), ((), ())), preferred_element_type=F32)


def diagonal(rows):
    row = lax.broadcasted_iota(jnp.int32, (rows, 128), 0)
    lane = lax.broadcasted_iota(jnp.int32, (rows, 128), 1)
    return lax.rem(lane, rows) == row


def attend_kernel(n_ref, q_ref, qm_ref, k_ref, km_ref, v_ref, o_ref, qa_scr, s_scr, m_scr, acc_scr, st_scr):
    tokens, kv_heads, group, width = q_ref.shape
    rows = tokens * group
    tile = rows // 2
    chunks = o_ref.shape[0]
    per = rows // chunks
    units = [(kv, slice(r, r + tile)) for kv in range(kv_heads) for r in range(0, rows, tile)]

    for kv in range(kv_heads):
        qa_scr[kv, :, :width] = q_ref[:, kv].reshape(rows, width)
        mask = jnp.broadcast_to(qm_ref[...][:, None, :], (tokens, group, 128))
        qa_scr[kv, :, width:] = mask.reshape(rows, 128).astype(BF16)

    @pl.loop(0, 2)
    def block(blk):
        def variant(slots):
            spans = [slice(c, min(c + CHUNK, slots)) for c in range(0, slots, CHUNK)]
            tops = []
            for kv, r in units:
                top = None
                for span in spans:
                    head = slice(kv * width, (kv + 1) * width)
                    k = jnp.concatenate([k_ref[blk, span, head], km_ref[blk, span, :]], axis=1)
                    s = dot_nt(qa_scr[kv, r], k)
                    s_scr[kv, r, span] = s
                    for l in range(0, s.shape[1], 128):
                        part = s[:, l : l + 128]
                        top = part if top is None else jnp.maximum(top, part)
                m_scr[blk, kv, r] = top
            for kv, r in units:
                top = jnp.max(m_scr[blk, kv, r], axis=1, keepdims=True)
                acc = None
                for span in spans:
                    p = jnp.exp2((s_scr[kv, r, span] - top) * LOG2_SCALE).astype(BF16)
                    v = v_ref[blk, span, kv * width : (kv + 1) * width]
                    term = dot_nn(p, jnp.concatenate([v, jnp.ones_like(v)], axis=1))
                    acc = term if acc is None else acc + term
                acc_scr[blk, kv, r] = acc
                m_scr[blk, kv, r] = jnp.broadcast_to(top * LOG2_SCALE, (tile, 128))

        used, low = n_ref[blk], 0
        full = k_ref.shape[1]
        for slots in (CHUNK, 2 * CHUNK, 3 * CHUNK, full):
            pl.when(jnp.logical_and(used > low, used <= slots))(functools.partial(variant, slots))
            low = slots

    @pl.loop(0, kv_heads)
    def close(kv):
        m_a, m_b = m_scr[0, kv], m_scr[1, kv]
        top = jnp.maximum(m_a, m_b)
        w_a, w_b = jnp.exp2(m_a - top), jnp.exp2(m_b - top)
        total = acc_scr[0, kv, :, width:] * w_a + acc_scr[1, kv, :, width:] * w_b
        mean = (acc_scr[0, kv, :, :width] * w_a + acc_scr[1, kv, :, :width] * w_b) / total
        lse = top + jnp.log2(total)
        at = pl.multiple_of(kv * per, per)
        coded, exponent = encode(mean)
        o_ref[:, pl.ds(at, per), :] = coded.reshape(chunks, per, width).astype(I16)
        pick = diagonal(per)[None]
        st_scr[0, kv] = jnp.sum(jnp.where(pick, lse.reshape(chunks, per, 128), 0.0), axis=1)
        spread = jnp.broadcast_to(exponent, (rows, 128)).reshape(chunks, per, 128)
        st_scr[1, kv] = jnp.sum(jnp.where(pick, spread, 0.0), axis=1)

    o_ref[:, kv_heads * per :, :] = stat_rows(
        [st_scr[0, kv] for kv in range(kv_heads)], [st_scr[1, kv] for kv in range(kv_heads)]
    )


def encode(mean):
    largest = jnp.max(jnp.abs(mean), axis=-1, keepdims=True)
    exponent = jnp.ceil(jnp.log2(jnp.maximum(largest, 1e-30)))
    return jnp.round(mean * (FULL * jnp.exp2(-exponent))).astype(I32), exponent


def stat_rows(lses, exponents):
    steps = [jnp.round(l * LSE_STEPS).astype(I32) for l in lses]
    terms = [lax.shift_right_arithmetic(t, jnp.full_like(t, 16)) for t in steps]
    terms += [(t & 0xFFFF) - 32768 for t in steps]
    terms += [e.astype(I32) for e in exponents]
    terms += [jnp.zeros_like(terms[0])] * (STAT_ROWS - len(terms))
    return jnp.stack(terms, axis=1).astype(I16)


def read_stats(stats):
    stats = stats.astype(I32)
    steps = stats[:, 0:2] * 65536 + (stats[:, 2:4] + 32768)
    return steps.astype(F32) * (1.0 / LSE_STEPS), jnp.exp2(stats[:, 4:6].astype(F32)) * (1.0 / FULL)


def as_column(w, per):
    chunks = w.shape[0]
    spread = jnp.broadcast_to(w[:, :, None, :], (chunks, 2, per, 128))
    lane = lax.broadcasted_iota(jnp.int32, (per, 128), 1)
    row = lax.broadcasted_iota(jnp.int32, (per, 128), 0)
    column = jnp.sum(jnp.where((lane == row)[None, None], spread, 0.0), axis=3, keepdims=True)
    return column.reshape(chunks, 2 * per, 1)


def numbers(coded):
    return coded.astype(I32).astype(F32)


def merge_kernel(*refs):
    pieces, o_ref = refs[:-1], refs[-1]
    rows = o_ref.shape[1] - STAT_ROWS
    per, at_once = rows // 2, 16

    for g in range(o_ref.shape[0] // at_once):
        here = slice(g * at_once, (g + 1) * at_once)
        lses, scales = zip(*[read_stats(p[here, rows:, :]) for p in pieces])
        top = functools.reduce(jnp.maximum, lses)
        weights = [jnp.exp2(l - top) for l in lses]
        total = functools.reduce(jnp.add, weights)
        lse = top + jnp.log2(total)
        out = None
        for p, w, scale in zip(pieces, weights, scales):
            term = numbers(p[here, :rows, :]) * as_column(w / total * scale, per)
            out = term if out is None else out + term
        coded, exponent = encode(out)
        o_ref[here, :rows, :] = coded.astype(I16)
        spread = jnp.broadcast_to(exponent, (at_once, rows, 128)).reshape(at_once, 2, per, 128)
        exponents = jnp.sum(jnp.where(diagonal(per)[None, None], spread, 0.0), axis=2)
        o_ref[here, rows:, :] = stat_rows([lse[:, kv] for kv in range(2)], [exponents[:, kv] for kv in range(2)])


def final_kernel(p_ref, o_ref):
    sources, rows, width = p_ref.shape
    rows -= STAT_ROWS
    lse, scale = read_stats(p_ref[:, rows:, :])
    lse = lse.reshape(sources // 2, 2, *lse.shape[1:])
    top = jnp.max(lse, axis=0, keepdims=True)
    weights = jnp.exp2(lse - top)
    weights = weights / jnp.sum(weights, axis=0, keepdims=True)
    column = as_column(weights.reshape(scale.shape) * scale, rows // 2)
    terms = (numbers(p_ref[:, :rows, :]) * column).reshape(sources // 2, 2 * rows, width)
    o_ref[...] = jnp.sum(terms, axis=0).astype(BF16)


VMEM_SPEC = pl.BlockSpec(memory_space=pltpu.VMEM)


def attend(counts, q, q_mask, keys, key_mask, values):
    tokens, kv_heads, group, width = q.shape
    rows = tokens * group
    slots = keys.shape[1]
    chunk_rows = kv_heads * group
    return pl.pallas_call(
        attend_kernel,
        out_shape=jax.ShapeDtypeStruct((tokens, chunk_rows + STAT_ROWS, width), I16),
        in_specs=[pl.BlockSpec(memory_space=pltpu.SMEM)] + [VMEM_SPEC] * 5,
        out_specs=VMEM_SPEC,
        scratch_shapes=[
            pltpu.VMEM((kv_heads, rows, width + 128), BF16),
            pltpu.VMEM((kv_heads, rows, slots), F32),
            pltpu.VMEM((2, kv_heads, rows, 128), F32),
            pltpu.VMEM((2, kv_heads, rows, 2 * width), F32),
            pltpu.VMEM((2, kv_heads, tokens, 128), F32),
        ],
        compiler_params=pltpu.CompilerParams(vmem_limit_bytes=32 * 1024 * 1024),
        cost_estimate=pl.CostEstimate(
            flops=4 * rows * kv_heads * slots * 2 * width,
            bytes_accessed=2 * (keys.size + values.size),
            transcendentals=rows * kv_heads * slots,
        ),
        name="attend",
    )(counts, q, q_mask, keys, key_mask, values)


def merge(pieces):
    return pl.pallas_call(
        merge_kernel,
        out_shape=jax.ShapeDtypeStruct(pieces[0].shape, I16),
        in_specs=[VMEM_SPEC] * len(pieces),
        out_specs=VMEM_SPEC,
        compiler_params=pltpu.CompilerParams(vmem_limit_bytes=8 * 1024 * 1024),
        cost_estimate=pl.CostEstimate(flops=8 * pieces[0].size, bytes_accessed=10 * pieces[0].size, transcendentals=0),
        name="merge",
    )(*pieces)


def finish(pieces):
    return pl.pallas_call(
        final_kernel,
        out_shape=jax.ShapeDtypeStruct((2 * (pieces.shape[1] - STAT_ROWS), HEAD_WIDTH), BF16),
        in_specs=[VMEM_SPEC],
        out_specs=VMEM_SPEC,
        compiler_params=pltpu.CompilerParams(vmem_limit_bytes=4 * 1024 * 1024),
        cost_estimate=pl.CostEstimate(flops=4 * pieces.size, bytes_accessed=2 * pieces.size, transcendentals=0),
        name="finish",
    )(pieces)


def along_x(a, step):
    return lax.ppermute(a, "x", [(i, (i - step) % NX) for i in range(NX)])


def body(queries, fresh_keys, fresh_values, cache_keys, stored_values, cache_lengths, positions):
    x, z, core = lax.axis_index("x"), lax.axis_index("z"), lax.axis_index("core")
    width, group = HEAD_WIDTH, HEADS_PER_GROUP
    kv_mine = fresh_keys.shape[1] // width // 2
    slots = cache_keys.shape[0]
    padded = slots + 128

    def half(a, which):
        size = a.shape[1] // 2
        return lax.dynamic_slice_in_dim(a, which * size, size, 1)

    with jax.named_scope("ask"):
        split = queries.reshape(1, 2, kv_mine, group, width)
        split = jnp.broadcast_to(split, (NZ, *split.shape[1:])).reshape(NZ * 2, kv_mine, group, width)
        column = lax.all_to_all(split, ("z", "core"), 0, 0, tiled=True)

    with jax.named_scope("swapped"):
        given = jnp.stack([half(cache_keys, 1 - core), half(stored_values, 1 - core)])
        kv_got = lax.ppermute(given, "core", SWAP)
    with jax.named_scope("newer"):
        fresh = jnp.concatenate([fresh_keys, fresh_values], axis=0)
        new = jnp.stack([half(fresh, core), lax.ppermute(half(fresh, 1 - core), "core", SWAP)])
    with jax.named_scope("lengths"):
        lengths = jnp.concatenate([cache_lengths, lax.ppermute(cache_lengths, "core", SWAP)])
    slot = jnp.arange(padded, dtype=I32)

    def extended(own, other, added):
        both = jnp.pad(jnp.stack([own, other]), ((0, 0), (0, padded - slots), (0, 0)))
        return jnp.where((slot[None, :] == lengths[:, None])[:, :, None], added[:, None, :], both)

    keys = extended(half(cache_keys, core), kv_got[0], new[:, 0])
    values = extended(half(stored_values, core), kv_got[1], new[:, 1])

    table = positions.reshape(NX, NZ * 2)
    here = lax.dynamic_slice(table, (x, z * 2), (1, 2)).reshape(2)
    here = jnp.where(core == 0, here, here[::-1])
    lane = jnp.arange(128, dtype=I32)
    new_lane = jnp.where(here > 0, here, -1)
    hide = jnp.where(slot[None, :] < lengths[:, None], -1, jnp.where(slot[None, :] == lengths[:, None], new_lane[:, None], 0))
    key_mask = jnp.where(lane[None, None, :] == hide[:, :, None], HIDDEN, 0.0).astype(BF16)
    counts = lengths + 1

    def q_mask(step):
        there = lax.dynamic_slice(table, (lax.rem(x + step, NX), 0), (1, NZ * 2)).reshape(NZ * 2, 1)
        return jnp.where((lane[None, :] > there) | (lane[None, :] == 0), 1.0, 0.0).astype(F32)

    steps = (0, 1, 3, 2)
    asked = [column if s == 0 else along_x(column, s) for s in steps]
    results = [attend(counts, q, q_mask(s), keys, key_mask, values) for q, s in zip(asked, steps)]
    pieces = [r if s == 0 else along_x(r, -s) for r, s in zip(results, steps)]
    merged = lax.all_to_all(merge(pieces), ("z", "core"), 0, 0, tiled=True)
    return finish(merged).reshape(1, -1)


def solution(mesh):
    finer = Mesh(mesh.devices.reshape(mesh.shape["groups"], NX, NZ, 2), GROUPS_CTX)
    return jax.shard_map(
        body,
        mesh=finer,
        in_specs=(
            P(GROUPS_CTX, None),
            P(GROUPS_CTX, None),
            P(GROUPS_CTX, None),
            P(GROUPS_CTX, None),
            P(GROUPS_CTX, None),
            P(GROUPS_CTX),
            P("groups"),
        ),
        out_specs=P(GROUPS_CTX, None),
        check_vma=False,
    )
```

```python
import functools
import math

import jax
import jax.numpy as jnp
from jax import lax
from jax.experimental import pallas as pl
from jax.experimental.pallas import tpu as pltpu
from jax.sharding import Mesh
from jax.sharding import PartitionSpec as P


HEADS_PER_GROUP = 16
HEAD_WIDTH = 128
GROUPS_CTX = ("groups", "x", "z", "core")
NX, NZ = 4, 16
LOG2_SCALE = HEAD_WIDTH ** (-0.5) * math.log2(math.e)
STAT_ROWS = 8
LSE_STEPS = 2.0**18
FULL = 32767.0
F32, BF16, I16, I32 = jnp.float32, jnp.bfloat16, jnp.int16, jnp.int32
SWAP = [(0, 1), (1, 0)]
CHUNK = 256
HIDDEN = -(2.0**100)


def dot_nt(a, b):
    return lax.dot_general(a, b, (((1,), (1,)), ((), ())), preferred_element_type=F32)


def dot_nn(a, b):
    return lax.dot_general(a, b, (((1,), (0,)), ((), ())), preferred_element_type=F32)


def diagonal(rows):
    row = lax.broadcasted_iota(jnp.int32, (rows, 128), 0)
    lane = lax.broadcasted_iota(jnp.int32, (rows, 128), 1)
    return lax.rem(lane, rows) == row


def attend_kernel(pieces, n_ref, k_ref, km_ref, v_ref, *refs):
    q_refs, qm_refs, o_refs = refs[:pieces], refs[pieces : 2 * pieces], refs[2 * pieces : 3 * pieces]
    qa_scr, s_scr, m_scr, acc_scr, st_scr = refs[3 * pieces :]
    tokens, kv_heads, group, width = q_refs[0].shape
    rows = tokens * group
    chunks = o_refs[0].shape[0]
    per = rows // chunks
    tile = rows // 2
    blocks = [(p, kv) for p in range(pieces) for kv in range(kv_heads)]
    units = [(h, kv, slice(r, r + tile)) for h, (p, kv) in enumerate(blocks) for r in range(0, rows, tile)]

    for h, (p, kv) in enumerate(blocks):
        qa_scr[h, :, :width] = q_refs[p][:, kv].reshape(rows, width)
        mask = jnp.broadcast_to(qm_refs[p][...][:, None, :], (tokens, group, 128))
        qa_scr[h, :, width:] = mask.reshape(rows, 128).astype(BF16)

    @pl.loop(0, 2)
    def block(blk):
        def variant(slots):
            spans = [slice(c, min(c + CHUNK, slots)) for c in range(0, slots, CHUNK)]
            for h, kv, r in units:
                top = None
                for span in spans:
                    head = slice(kv * width, (kv + 1) * width)
                    k = jnp.concatenate([k_ref[blk, span, head], km_ref[blk, span, :]], axis=1)
                    s = dot_nt(qa_scr[h, r], k)
                    s_scr[h, r, span] = s
                    for l in range(0, s.shape[1], 128):
                        part = s[:, l : l + 128]
                        top = part if top is None else jnp.maximum(top, part)
                m_scr[blk, h, r] = top
            for h, kv, r in units:
                top = jnp.max(m_scr[blk, h, r], axis=1, keepdims=True)
                acc = None
                for span in spans:
                    p = jnp.exp2((s_scr[h, r, span] - top) * LOG2_SCALE).astype(BF16)
                    v = v_ref[blk, span, kv * width : (kv + 1) * width]
                    term = dot_nn(p, jnp.concatenate([v, jnp.ones_like(v)], axis=1))
                    acc = term if acc is None else acc + term
                acc_scr[blk, h, r] = acc
                m_scr[blk, h, r] = jnp.broadcast_to(top * LOG2_SCALE, (tile, 128))

        used, low = n_ref[blk], 0
        full = k_ref.shape[1]
        for slots in (CHUNK, 2 * CHUNK, 3 * CHUNK, full):
            pl.when(jnp.logical_and(used > low, used <= slots))(functools.partial(variant, slots))
            low = slots

    for p in range(pieces):

        @pl.loop(0, kv_heads)
        def close(kv, p=p):
            h = p * kv_heads + kv
            m_a, m_b = m_scr[0, h], m_scr[1, h]
            top = jnp.maximum(m_a, m_b)
            w_a, w_b = jnp.exp2(m_a - top), jnp.exp2(m_b - top)
            total = acc_scr[0, h, :, width:] * w_a + acc_scr[1, h, :, width:] * w_b
            mean = (acc_scr[0, h, :, :width] * w_a + acc_scr[1, h, :, :width] * w_b) / total
            lse = top + jnp.log2(total)
            at = pl.multiple_of(kv * per, per)
            coded, exponent = encode(mean)
            o_refs[p][:, pl.ds(at, per), :] = coded.reshape(chunks, per, width).astype(I16)
            pick = diagonal(per)[None]
            st_scr[0, kv] = jnp.sum(jnp.where(pick, lse.reshape(chunks, per, 128), 0.0), axis=1)
            spread = jnp.broadcast_to(exponent, (rows, 128)).reshape(chunks, per, 128)
            st_scr[1, kv] = jnp.sum(jnp.where(pick, spread, 0.0), axis=1)

        o_refs[p][:, kv_heads * per :, :] = stat_rows(
            [st_scr[0, kv] for kv in range(kv_heads)], [st_scr[1, kv] for kv in range(kv_heads)]
        )


def encode(mean):
    largest = jnp.max(jnp.abs(mean), axis=-1, keepdims=True)
    exponent = jnp.ceil(jnp.log2(jnp.maximum(largest, 1e-30)))
    return jnp.round(mean * (FULL * jnp.exp2(-exponent))).astype(I32), exponent


def stat_rows(lses, exponents):
    steps = [jnp.round(l * LSE_STEPS).astype(I32) for l in lses]
    terms = [lax.shift_right_arithmetic(t, jnp.full_like(t, 16)) for t in steps]
    terms += [(t & 0xFFFF) - 32768 for t in steps]
    terms += [e.astype(I32) for e in exponents]
    terms += [jnp.zeros_like(terms[0])] * (STAT_ROWS - len(terms))
    return jnp.stack(terms, axis=1).astype(I16)


def read_stats(stats):
    stats = stats.astype(I32)
    steps = stats[:, 0:2] * 65536 + (stats[:, 2:4] + 32768)
    return steps.astype(F32) * (1.0 / LSE_STEPS), jnp.exp2(stats[:, 4:6].astype(F32)) * (1.0 / FULL)


def as_column(w, per):
    chunks = w.shape[0]
    spread = jnp.broadcast_to(w[:, :, None, :], (chunks, 2, per, 128))
    lane = lax.broadcasted_iota(jnp.int32, (per, 128), 1)
    row = lax.broadcasted_iota(jnp.int32, (per, 128), 0)
    column = jnp.sum(jnp.where((lane == row)[None, None], spread, 0.0), axis=3, keepdims=True)
    return column.reshape(chunks, 2 * per, 1)


def numbers(coded):
    return coded.astype(I32).astype(F32)


def merge_kernel(*refs):
    pieces, o_ref = refs[:-1], refs[-1]
    rows = o_ref.shape[1] - STAT_ROWS
    per, at_once = rows // 2, 16

    for g in range(o_ref.shape[0] // at_once):
        here = slice(g * at_once, (g + 1) * at_once)
        lses, scales = zip(*[read_stats(p[here, rows:, :]) for p in pieces])
        top = functools.reduce(jnp.maximum, lses)
        weights = [jnp.exp2(l - top) for l in lses]
        total = functools.reduce(jnp.add, weights)
        lse = top + jnp.log2(total)
        out = None
        for p, w, scale in zip(pieces, weights, scales):
            term = numbers(p[here, :rows, :]) * as_column(w / total * scale, per)
            out = term if out is None else out + term
        coded, exponent = encode(out)
        o_ref[here, :rows, :] = coded.astype(I16)
        spread = jnp.broadcast_to(exponent, (at_once, rows, 128)).reshape(at_once, 2, per, 128)
        exponents = jnp.sum(jnp.where(diagonal(per)[None, None], spread, 0.0), axis=2)
        o_ref[here, rows:, :] = stat_rows([lse[:, kv] for kv in range(2)], [exponents[:, kv] for kv in range(2)])


def final_kernel(core_ref, p_ref, own_ref, other_ref, scr):
    rows = p_ref.shape[1] - STAT_ROWS
    group = rows // 4
    lse, scale = read_stats(p_ref[:, rows:, :])
    top = jnp.max(lse, axis=0, keepdims=True)
    weights = jnp.exp2(lse - top)
    weights = weights / jnp.sum(weights, axis=0, keepdims=True)
    column = as_column(weights * scale, rows // 2)
    out = jnp.sum(numbers(p_ref[:, :rows, :]) * column, axis=0).astype(BF16)
    for kv in range(2):
        for token in range(2):
            at = (2 * kv + token) * group
            scr[token, kv * group : (kv + 1) * group] = out[at : at + group]
    own_ref[...] = scr[core_ref[0]]
    other_ref[...] = scr[1 - core_ref[0]]


VMEM_SPEC = pl.BlockSpec(memory_space=pltpu.VMEM)


def attend(counts, qs, q_masks, keys, key_mask, values):
    tokens, kv_heads, group, width = qs[0].shape
    rows = tokens * group
    slots = keys.shape[1]
    pieces = len(qs)
    out = jax.ShapeDtypeStruct((NZ, tokens // NZ * kv_heads * group + STAT_ROWS, width), I16)
    return pl.pallas_call(
        functools.partial(attend_kernel, pieces),
        out_shape=[out] * pieces,
        in_specs=[pl.BlockSpec(memory_space=pltpu.SMEM)] + [VMEM_SPEC] * (3 + 2 * pieces),
        out_specs=[VMEM_SPEC] * pieces,
        scratch_shapes=[
            pltpu.VMEM((pieces * kv_heads, rows, width + 128), BF16),
            pltpu.VMEM((pieces * kv_heads, rows, slots), F32),
            pltpu.VMEM((2, pieces * kv_heads, rows, 128), F32),
            pltpu.VMEM((2, pieces * kv_heads, rows, 2 * width), F32),
            pltpu.VMEM((2, kv_heads, NZ, 128), F32),
        ],
        compiler_params=pltpu.CompilerParams(vmem_limit_bytes=32 * 1024 * 1024),
        cost_estimate=pl.CostEstimate(
            flops=4 * pieces * rows * kv_heads * slots * 2 * width,
            bytes_accessed=2 * (keys.size + values.size),
            transcendentals=pieces * rows * kv_heads * slots,
        ),
        name="attend",
    )(counts, keys, key_mask, values, *qs, *q_masks)


def merge(pieces):
    return pl.pallas_call(
        merge_kernel,
        out_shape=jax.ShapeDtypeStruct(pieces[0].shape, I16),
        in_specs=[VMEM_SPEC] * len(pieces),
        out_specs=VMEM_SPEC,
        compiler_params=pltpu.CompilerParams(vmem_limit_bytes=8 * 1024 * 1024),
        cost_estimate=pl.CostEstimate(flops=8 * pieces[0].size, bytes_accessed=10 * pieces[0].size, transcendentals=0),
        name="merge",
    )(*pieces)


def finish(core, pieces):
    half = jax.ShapeDtypeStruct(((pieces.shape[1] - STAT_ROWS) // 2, HEAD_WIDTH), BF16)
    return pl.pallas_call(
        final_kernel,
        out_shape=[half, half],
        in_specs=[pl.BlockSpec(memory_space=pltpu.SMEM), VMEM_SPEC],
        out_specs=[VMEM_SPEC, VMEM_SPEC],
        scratch_shapes=[pltpu.VMEM((2, *half.shape), BF16)],
        compiler_params=pltpu.CompilerParams(vmem_limit_bytes=4 * 1024 * 1024),
        cost_estimate=pl.CostEstimate(flops=4 * pieces.size, bytes_accessed=2 * pieces.size, transcendentals=0),
        name="finish",
    )(core.reshape(1), pieces)


def along_x(a, step):
    return lax.ppermute(a, "x", [(i, (i - step) % NX) for i in range(NX)])


def body(queries, fresh_keys, fresh_values, cache_keys, stored_values, cache_lengths, positions):
    x, z, core = lax.axis_index("x"), lax.axis_index("z"), lax.axis_index("core")
    width, group = HEAD_WIDTH, HEADS_PER_GROUP
    kv_mine = fresh_keys.shape[1] // width // 2
    slots = cache_keys.shape[0]
    padded = slots + 128

    def half(a, which):
        size = a.shape[1] // 2
        return lax.dynamic_slice_in_dim(a, which * size, size, 1)

    split = queries.reshape(1, 2, kv_mine, group, width)
    split = jnp.broadcast_to(split, (NZ, *split.shape[1:])).reshape(NZ * 2, kv_mine, group, width)
    column = lax.all_to_all(split, ("z", "core"), 0, 0, tiled=True)

    given = jnp.stack([half(cache_keys, 1 - core), half(stored_values, 1 - core)])
    kv_got = lax.ppermute(given, "core", SWAP)
    fresh = jnp.concatenate([fresh_keys, fresh_values], axis=0)
    new = jnp.stack([half(fresh, core), lax.ppermute(half(fresh, 1 - core), "core", SWAP)])
    lengths = jnp.concatenate([cache_lengths, lax.ppermute(cache_lengths, "core", SWAP)])
    slot = jnp.arange(padded, dtype=I32)

    def extended(own, other, added):
        both = jnp.pad(jnp.stack([own, other]), ((0, 0), (0, padded - slots), (0, 0)))
        return jnp.where((slot[None, :] == lengths[:, None])[:, :, None], added[:, None, :], both)

    keys = extended(half(cache_keys, core), kv_got[0], new[:, 0])
    values = extended(half(stored_values, core), kv_got[1], new[:, 1])

    table = positions.reshape(NX, NZ * 2)
    here = lax.dynamic_slice(table, (x, z * 2), (1, 2)).reshape(2)
    here = jnp.where(core == 0, here, here[::-1])
    lane = jnp.arange(128, dtype=I32)
    new_lane = jnp.where(here > 0, here, -1)
    hide = jnp.where(slot[None, :] < lengths[:, None], -1, jnp.where(slot[None, :] == lengths[:, None], new_lane[:, None], 0))
    key_mask = jnp.where(lane[None, None, :] == hide[:, :, None], HIDDEN, 0.0).astype(BF16)
    counts = lengths + 1

    def q_mask(step):
        there = lax.dynamic_slice(table, (lax.rem(x + step, NX), 0), (1, NZ * 2)).reshape(NZ * 2, 1)
        return jnp.where((lane[None, :] > there) | (lane[None, :] == 0), 1.0, 0.0).astype(F32)

    def results(*steps):
        asked = [column if s == 0 else along_x(column, s) for s in steps]
        return attend(counts, asked, [q_mask(s) for s in steps], keys, key_mask, values)

    next_to, before = results(1, NX - 1)
    (across,) = results(NX // 2)
    (own,) = results(0)
    merged = merge([own, along_x(next_to, -1), along_x(before, 1), along_x(across, -(NX // 2))])
    mine, other = finish(core, lax.all_to_all(merged, "z", 0, 0, tiled=True))
    back = lax.ppermute(other, "core", SWAP)
    first, second = jnp.where(core == 0, mine, back), jnp.where(core == 0, back, mine)
    return jnp.concatenate([first, second], axis=0).reshape(1, -1)


def solution(mesh):
    finer = Mesh(mesh.devices.reshape(mesh.shape["groups"], NX, NZ, 2), GROUPS_CTX)
    return jax.shard_map(
        body,
        mesh=finer,
        in_specs=(
            P(GROUPS_CTX, None),
            P(GROUPS_CTX, None),
            P(GROUPS_CTX, None),
            P(GROUPS_CTX, None),
            P(GROUPS_CTX, None),
            P(GROUPS_CTX),
            P("groups"),
        ),
        out_specs=P(GROUPS_CTX, None),
        check_vma=False,
    )
```

```python
import functools
import math

import jax
import jax.numpy as jnp
from jax import lax
from jax.experimental import pallas as pl
from jax.experimental.pallas import tpu as pltpu
from jax.sharding import Mesh
from jax.sharding import PartitionSpec as P


HEADS_PER_GROUP = 16
HEAD_WIDTH = 128
GROUPS_CTX = ("groups", "x", "z", "core")
NX, NZ = 4, 16
LOG2_SCALE = HEAD_WIDTH ** (-0.5) * math.log2(math.e)
STAT_ROWS = 8
LSE_STEPS = 2.0**18
FULL = 32767.0
F32, BF16, I16, I32 = jnp.float32, jnp.bfloat16, jnp.int16, jnp.int32
SWAP = [(0, 1), (1, 0)]
CHUNK = 256
HIDDEN = -(2.0**100)


def dot_nt(a, b):
    return lax.dot_general(a, b, (((1,), (1,)), ((), ())), preferred_element_type=F32)


def dot_nn(a, b):
    return lax.dot_general(a, b, (((1,), (0,)), ((), ())), preferred_element_type=F32)


def diagonal(rows):
    row = lax.broadcasted_iota(jnp.int32, (rows, 128), 0)
    lane = lax.broadcasted_iota(jnp.int32, (rows, 128), 1)
    return lax.rem(lane, rows) == row


def attend_kernel(pieces, n_ref, k_ref, km_ref, v_ref, *refs):
    q_refs, qm_refs, o_refs = refs[:pieces], refs[pieces : 2 * pieces], refs[2 * pieces : 3 * pieces]
    qa_scr, s_scr, m_scr, acc_scr, st_scr = refs[3 * pieces :]
    tokens, kv_heads, group, width = q_refs[0].shape
    rows = tokens * group
    chunks = o_refs[0].shape[0]
    per = rows // chunks
    tile = rows // 2
    blocks = [(p, kv) for p in range(pieces) for kv in range(kv_heads)]
    units = [(h, kv, slice(r, r + tile)) for h, (p, kv) in enumerate(blocks) for r in range(0, rows, tile)]

    for h, (p, kv) in enumerate(blocks):
        qa_scr[h, :, :width] = q_refs[p][:, kv].reshape(rows, width)
        mask = jnp.broadcast_to(qm_refs[p][...][:, None, :], (tokens, group, 128))
        qa_scr[h, :, width:] = mask.reshape(rows, 128).astype(BF16)

    @pl.loop(0, 2)
    def block(blk):
        def variant(slots):
            spans = [slice(c, min(c + CHUNK, slots)) for c in range(0, slots, CHUNK)]
            for h, kv, r in units:
                top = None
                for span in spans:
                    head = slice(kv * width, (kv + 1) * width)
                    k = jnp.concatenate([k_ref[blk, span, head], km_ref[blk, span, :]], axis=1)
                    s = dot_nt(qa_scr[h, r], k)
                    s_scr[h, r, span] = s
                    for l in range(0, s.shape[1], 128):
                        part = s[:, l : l + 128]
                        top = part if top is None else jnp.maximum(top, part)
                m_scr[blk, h, r] = top
            for h, kv, r in units:
                top = jnp.max(m_scr[blk, h, r], axis=1, keepdims=True)
                acc = None
                for span in spans:
                    p = jnp.exp2((s_scr[h, r, span] - top) * LOG2_SCALE).astype(BF16)
                    v = v_ref[blk, span, kv * width : (kv + 1) * width]
                    term = dot_nn(p, jnp.concatenate([v, jnp.ones_like(v)], axis=1))
                    acc = term if acc is None else acc + term
                acc_scr[blk, h, r] = acc
                m_scr[blk, h, r] = jnp.broadcast_to(top * LOG2_SCALE, (tile, 128))

        used, low = n_ref[blk], 0
        full = k_ref.shape[1]
        for slots in (CHUNK, 2 * CHUNK, 3 * CHUNK, full):
            pl.when(jnp.logical_and(used > low, used <= slots))(functools.partial(variant, slots))
            low = slots

    for p in range(pieces):

        @pl.loop(0, kv_heads)
        def close(kv, p=p):
            h = p * kv_heads + kv
            m_a, m_b = m_scr[0, h], m_scr[1, h]
            top = jnp.maximum(m_a, m_b)
            w_a, w_b = jnp.exp2(m_a - top), jnp.exp2(m_b - top)
            total = acc_scr[0, h, :, width:] * w_a + acc_scr[1, h, :, width:] * w_b
            mean = (acc_scr[0, h, :, :width] * w_a + acc_scr[1, h, :, :width] * w_b) / total
            lse = top + jnp.log2(total)
            at = pl.multiple_of(kv * per, per)
            coded, exponent = encode(mean)
            o_refs[p][:, pl.ds(at, per), :] = coded.reshape(chunks, per, width).astype(I16)
            pick = diagonal(per)[None]
            st_scr[0, kv] = jnp.sum(jnp.where(pick, lse.reshape(chunks, per, 128), 0.0), axis=1)
            spread = jnp.broadcast_to(exponent, (rows, 128)).reshape(chunks, per, 128)
            st_scr[1, kv] = jnp.sum(jnp.where(pick, spread, 0.0), axis=1)

        o_refs[p][:, kv_heads * per :, :] = stat_rows(
            [st_scr[0, kv] for kv in range(kv_heads)], [st_scr[1, kv] for kv in range(kv_heads)]
        )


def encode(mean):
    largest = jnp.max(jnp.abs(mean), axis=-1, keepdims=True)
    exponent = jnp.ceil(jnp.log2(jnp.maximum(largest, 1e-30)))
    return jnp.round(mean * (FULL * jnp.exp2(-exponent))).astype(I32), exponent


def stat_rows(lses, exponents):
    steps = [jnp.round(l * LSE_STEPS).astype(I32) for l in lses]
    terms = [lax.shift_right_arithmetic(t, jnp.full_like(t, 16)) for t in steps]
    terms += [(t & 0xFFFF) - 32768 for t in steps]
    terms += [e.astype(I32) for e in exponents]
    terms += [jnp.zeros_like(terms[0])] * (STAT_ROWS - len(terms))
    return jnp.stack(terms, axis=1).astype(I16)


def read_stats(stats):
    stats = stats.astype(I32)
    steps = stats[:, 0:2] * 65536 + (stats[:, 2:4] + 32768)
    return steps.astype(F32) * (1.0 / LSE_STEPS), jnp.exp2(stats[:, 4:6].astype(F32)) * (1.0 / FULL)


def as_column(w, per):
    chunks = w.shape[0]
    spread = jnp.broadcast_to(w[:, :, None, :], (chunks, 2, per, 128))
    lane = lax.broadcasted_iota(jnp.int32, (per, 128), 1)
    row = lax.broadcasted_iota(jnp.int32, (per, 128), 0)
    column = jnp.sum(jnp.where((lane == row)[None, None], spread, 0.0), axis=3, keepdims=True)
    return column.reshape(chunks, 2 * per, 1)


def numbers(coded):
    return coded.astype(I32).astype(F32)


def merge_kernel(*refs):
    pieces, o_ref = refs[:-1], refs[-1]
    rows = o_ref.shape[1] - STAT_ROWS
    per, at_once = rows // 2, 16

    for g in range(o_ref.shape[0] // at_once):
        here = slice(g * at_once, (g + 1) * at_once)
        lses, scales = zip(*[read_stats(p[here, rows:, :]) for p in pieces])
        top = functools.reduce(jnp.maximum, lses)
        weights = [jnp.exp2(l - top) for l in lses]
        total = functools.reduce(jnp.add, weights)
        lse = top + jnp.log2(total)
        out = None
        for p, w, scale in zip(pieces, weights, scales):
            term = numbers(p[here, :rows, :]) * as_column(w / total * scale, per)
            out = term if out is None else out + term
        coded, exponent = encode(out)
        o_ref[here, :rows, :] = coded.astype(I16)
        spread = jnp.broadcast_to(exponent, (at_once, rows, 128)).reshape(at_once, 2, per, 128)
        exponents = jnp.sum(jnp.where(diagonal(per)[None, None], spread, 0.0), axis=2)
        o_ref[here, rows:, :] = stat_rows([lse[:, kv] for kv in range(2)], [exponents[:, kv] for kv in range(2)])


def final_kernel(core_ref, p_ref, own_ref, other_ref, scr):
    rows = p_ref.shape[1] - STAT_ROWS
    group = rows // 4
    lse, scale = read_stats(p_ref[:, rows:, :])
    top = jnp.max(lse, axis=0, keepdims=True)
    weights = jnp.exp2(lse - top)
    weights = weights / jnp.sum(weights, axis=0, keepdims=True)
    column = as_column(weights * scale, rows // 2)
    out = jnp.sum(numbers(p_ref[:, :rows, :]) * column, axis=0).astype(BF16)
    for kv in range(2):
        for token in range(2):
            at = (2 * kv + token) * group
            scr[token, kv * group : (kv + 1) * group] = out[at : at + group]
    own_ref[...] = scr[core_ref[0]]
    other_ref[...] = scr[1 - core_ref[0]]


VMEM_SPEC = pl.BlockSpec(memory_space=pltpu.VMEM)


def attend(counts, qs, q_masks, keys, key_mask, values):
    tokens, kv_heads, group, width = qs[0].shape
    rows = tokens * group
    slots = keys.shape[1]
    pieces = len(qs)
    out = jax.ShapeDtypeStruct((NZ, tokens // NZ * kv_heads * group + STAT_ROWS, width), I16)
    return pl.pallas_call(
        functools.partial(attend_kernel, pieces),
        out_shape=[out] * pieces,
        in_specs=[pl.BlockSpec(memory_space=pltpu.SMEM)] + [VMEM_SPEC] * (3 + 2 * pieces),
        out_specs=[VMEM_SPEC] * pieces,
        scratch_shapes=[
            pltpu.VMEM((pieces * kv_heads, rows, width + 128), BF16),
            pltpu.VMEM((pieces * kv_heads, rows, slots), F32),
            pltpu.VMEM((2, pieces * kv_heads, rows, 128), F32),
            pltpu.VMEM((2, pieces * kv_heads, rows, 2 * width), F32),
            pltpu.VMEM((2, kv_heads, NZ, 128), F32),
        ],
        compiler_params=pltpu.CompilerParams(vmem_limit_bytes=32 * 1024 * 1024),
        cost_estimate=pl.CostEstimate(
            flops=4 * pieces * rows * kv_heads * slots * 2 * width,
            bytes_accessed=2 * (keys.size + values.size),
            transcendentals=pieces * rows * kv_heads * slots,
        ),
        name="attend",
    )(counts, keys, key_mask, values, *qs, *q_masks)


def merge(pieces):
    return pl.pallas_call(
        merge_kernel,
        out_shape=jax.ShapeDtypeStruct(pieces[0].shape, I16),
        in_specs=[VMEM_SPEC] * len(pieces),
        out_specs=VMEM_SPEC,
        compiler_params=pltpu.CompilerParams(vmem_limit_bytes=8 * 1024 * 1024),
        cost_estimate=pl.CostEstimate(flops=8 * pieces[0].size, bytes_accessed=10 * pieces[0].size, transcendentals=0),
        name="merge",
    )(*pieces)


def finish(core, pieces):
    half = jax.ShapeDtypeStruct(((pieces.shape[1] - STAT_ROWS) // 2, HEAD_WIDTH), BF16)
    return pl.pallas_call(
        final_kernel,
        out_shape=[half, half],
        in_specs=[pl.BlockSpec(memory_space=pltpu.SMEM), VMEM_SPEC],
        out_specs=[VMEM_SPEC, VMEM_SPEC],
        scratch_shapes=[pltpu.VMEM((2, *half.shape), BF16)],
        compiler_params=pltpu.CompilerParams(vmem_limit_bytes=4 * 1024 * 1024),
        cost_estimate=pl.CostEstimate(flops=4 * pieces.size, bytes_accessed=2 * pieces.size, transcendentals=0),
        name="finish",
    )(core.reshape(1), pieces)


def along_x(a, step):
    return lax.ppermute(a, "x", [(i, (i - step) % NX) for i in range(NX)])


def body(queries, fresh_keys, fresh_values, cache_keys, stored_values, cache_lengths, positions):
    x, z, core = lax.axis_index("x"), lax.axis_index("z"), lax.axis_index("core")
    width, group = HEAD_WIDTH, HEADS_PER_GROUP
    kv_mine = fresh_keys.shape[1] // width // 2
    slots = cache_keys.shape[0]
    padded = slots + 128

    def half(a, which):
        size = a.shape[1] // 2
        return lax.dynamic_slice_in_dim(a, which * size, size, 1)

    split = queries.reshape(1, 2, kv_mine, group, width)
    split = jnp.broadcast_to(split, (NZ, *split.shape[1:])).reshape(NZ * 2, kv_mine, group, width)
    column = lax.all_to_all(split, ("z", "core"), 0, 0, tiled=True)

    given = jnp.stack([half(cache_keys, 1 - core), half(stored_values, 1 - core)])
    kv_got = lax.ppermute(given, "core", SWAP)
    fresh = jnp.concatenate([fresh_keys, fresh_values], axis=0)
    new = jnp.stack([half(fresh, core), lax.ppermute(half(fresh, 1 - core), "core", SWAP)])
    lengths = jnp.concatenate([cache_lengths, lax.ppermute(cache_lengths, "core", SWAP)])
    slot = jnp.arange(padded, dtype=I32)

    def extended(own, other, added):
        both = jnp.pad(jnp.stack([own, other]), ((0, 0), (0, padded - slots), (0, 0)))
        return jnp.where((slot[None, :] == lengths[:, None])[:, :, None], added[:, None, :], both)

    keys = extended(half(cache_keys, core), kv_got[0], new[:, 0])
    values = extended(half(stored_values, core), kv_got[1], new[:, 1])

    table = positions.reshape(NX, NZ * 2)
    here = lax.dynamic_slice(table, (x, z * 2), (1, 2)).reshape(2)
    here = jnp.where(core == 0, here, here[::-1])
    lane = jnp.arange(128, dtype=I32)
    new_lane = jnp.where(here > 0, here, -1)
    hide = jnp.where(slot[None, :] < lengths[:, None], -1, jnp.where(slot[None, :] == lengths[:, None], new_lane[:, None], 0))
    key_mask = jnp.where(lane[None, None, :] == hide[:, :, None], HIDDEN, 0.0).astype(BF16)
    counts = lengths + 1

    def q_mask(step):
        there = lax.dynamic_slice(table, (lax.rem(x + step, NX), 0), (1, NZ * 2)).reshape(NZ * 2, 1)
        return jnp.where((lane[None, :] > there) | (lane[None, :] == 0), 1.0, 0.0).astype(F32)

    def fetched(step):
        return along_x(column, step)

    def results(*steps):
        asked = [column if s == 0 else fetched(s) for s in steps]
        return attend(counts, asked, [q_mask(s) for s in steps], keys, key_mask, values)

    (next_to,) = results(1)
    (before,) = results(NX - 1)
    (across,) = results(NX // 2)
    (own,) = results(0)

    def returned(a, step):
        return along_x(a, -step)

    merged = merge([own, returned(next_to, 1), returned(before, NX - 1), returned(across, NX // 2)])
    mine, other = finish(core, lax.all_to_all(merged, "z", 0, 0, tiled=True))
    back = lax.ppermute(other, "core", SWAP)
    first, second = jnp.where(core == 0, mine, back), jnp.where(core == 0, back, mine)
    return jnp.concatenate([first, second], axis=0).reshape(1, -1)


def solution(mesh):
    finer = Mesh(mesh.devices.reshape(mesh.shape["groups"], NX, NZ, 2), GROUPS_CTX)
    return jax.shard_map(
        body,
        mesh=finer,
        in_specs=(
            P(GROUPS_CTX, None),
            P(GROUPS_CTX, None),
            P(GROUPS_CTX, None),
            P(GROUPS_CTX, None),
            P(GROUPS_CTX, None),
            P(GROUPS_CTX),
            P("groups"),
        ),
        out_specs=P(GROUPS_CTX, None),
        check_vma=False,
    )
```
